32 devices in a mesh: sx: 4 (over x, core), sy: 2 (over y), px: 4 (over z).
Axes of the slice: x: 2, y: 2, z: 4, core: 2. Of those that a mesh axis runs over, the one named last changes fastest.
Arguments:
- patterns: bfloat16 [64, 64, 9216], P('sx', 'sy', 'px'), may hold values from -6 to 6
- basis: bfloat16 [9216, 256], P('px', ('sx', 'sy')), may hold values from -0.375 to 0.375
- valid: int32 [64, 64], P('sx', 'sy'), may hold values 0 or 1
- strength: float32 [64, 64], P('sx', 'sy'), may hold values from 0.25 to 2
Outputs:
- denoised: bfloat16 [64, 64, 9216], P('sx', 'sy', 'px')
The draws below stay inside these ranges and needn't reach their ends.
Inputs may be any that keep to these rules, and one draw needn't show every extreme that they name: `valid`: 1 marks an on-sample scan position, 0 an off-sample one.
All inputs are finite; a program needn't handle non-finite values. No bound on the sum of `valid` on one device may be relied on, other than what follows from the above.
Results may differ from the reference program's by a relative error of at most 0.0089.
Values may be sent and summed in bfloat16 or wider, within the bound.
No kernel may reach another device: no remote copies, remote signals or barrier semaphores. Data moves between devices by JAX's collectives and lax.ppermute only.
A program may use at most 64 MiB of HBM per device.

```python
import math
import jax
import jax.numpy as jnp
from jax import lax

PIX = 9216
RANK = 256
RADIUS = 3
NX = 64
NY = 64


def touch_ends(entries, own_key, least, top_value):
    longest = entries.shape.index(max(entries.shape))
    spots = []
    for shift in (0, 1):
        where = [jax.random.randint(jax.random.fold_in(own_key, axis), (), 0, length) for axis, length in enumerate(entries.shape)]
        where[longest] = (where[longest] + shift) % entries.shape[longest]
        spots.append(tuple(where))
    return entries.at[spots[0]].set(least).at[spots[1]].set(top_value)


def steps_of(stream_key, dims, split, least, largest):
    def one(axis_at, shards_of):
        steps = jax.random.uniform(jax.random.fold_in(jax.random.fold_in(stream_key, 6), axis_at), (shards_of,), jnp.float32, least / len(split), largest / len(split))
        return jnp.repeat(jnp.exp(steps), dims[axis_at] // shards_of).reshape((-1,) + (1,) * (len(dims) - axis_at - 1))

    level = one(*split[0])
    for cut in split[1:]:
        level = level * one(*cut)
    return level


def gaussian(stream_key, extent, scale, reach, shards=(), dtype=jnp.bfloat16):
    drawn = scale * jax.random.normal(stream_key, extent, jnp.float32)
    if shards:
        drawn = drawn * steps_of(stream_key, extent, shards, -0.22, 0.18)
    return jnp.clip(drawn, -reach, reach).astype(dtype)


def setup_inputs(seed: int = 0) -> dict:
    key_list = jax.random.split(jax.random.key(seed), 5)
    return {
        "patterns": gaussian(key_list[0], (NX, NY, PIX), 1.0, 6.0, ((0, 4), (1, 2), (2, 4))),
        "basis": gaussian(key_list[1], (PIX, RANK), RANK ** -0.5, 0.375, ((0, 4), (1, 8))),
        "valid": touch_ends((jax.random.randint(key_list[2], (NX, NY), 0, 8) < 7).astype(jnp.int32), jax.random.fold_in(key_list[2], 1), 0, 1),
        "strength": jnp.clip(jnp.exp(math.log(2.0) - 2.0794415 * jax.random.uniform(key_list[3], (NX, NY), jnp.float32) ** steps_of(key_list[3], (NX, NY), ((0, 4), (1, 2)), -0.2, 0.2)), 0.25, 2.0),
    }


def neighbour_steps():
    steps = []
    for row_step in range(-RADIUS, RADIUS + 1):
        for col_step in range(-RADIUS, RADIUS + 1):
            if row_step != 0 or col_step != 0:
                steps.append((row_step, col_step))
    return steps


def squared_gaps(center, padded):
    rows, cols = center.shape[0], center.shape[1]
    gaps = []
    for row_step, col_step in neighbour_steps():
        other = padded[RADIUS + row_step:RADIUS + row_step + rows, RADIUS + col_step:RADIUS + col_step + cols]
        differ = center - other
        gaps.append(jnp.sum(differ * differ, axis=-1))
    return jnp.stack(gaps)


def blend(center, padded, mask_pad, gaps, strength):
    rows, cols = center.shape[0], center.shape[1]
    factor = 1.0 / (2.0 * PIX * strength)
    numerator = center
    total = jnp.ones((rows, cols), jnp.float32)
    for index, (row_step, col_step) in enumerate(neighbour_steps()):
        other = padded[RADIUS + row_step:RADIUS + row_step + rows, RADIUS + col_step:RADIUS + col_step + cols]
        mask_other = mask_pad[RADIUS + row_step:RADIUS + row_step + rows, RADIUS + col_step:RADIUS + col_step + cols]
        weight = mask_other * jnp.exp(-gaps[index] * factor)
        numerator = numerator + weight[:, :, None] * other
        total = total + weight
    return numerator / total[:, :, None]


def reference(patterns, basis, valid, strength):
    def project(row_block):
        return jnp.dot(row_block, basis, preferred_element_type=jnp.float32)

    coeffs = lax.map(project, patterns)
    mask_full = valid.astype(jnp.float32)
    padded = jnp.pad(coeffs, ((RADIUS, RADIUS), (RADIUS, RADIUS), (0, 0)))
    mask_pad = jnp.pad(mask_full, ((RADIUS, RADIUS), (RADIUS, RADIUS)))
    gaps = squared_gaps(coeffs, padded)
    average = blend(coeffs, padded, mask_pad, gaps, strength).astype(jnp.bfloat16)

    def rebuild(row_block):
        product = lax.dot_general(row_block, basis, (((1,), (1,)), ((), ())), preferred_element_type=jnp.float32)
        return product.astype(jnp.bfloat16)

    return lax.map(rebuild, average)
```

```python
import functools

import jax
import jax.numpy as jnp
from jax import lax
from jax.experimental import pallas as pl
from jax.experimental.pallas import tpu as pltpu
from jax.sharding import PartitionSpec as P

RADIUS = 3
STRIP = 16
OFF = 2.0**40
F32, BF16 = jnp.float32, jnp.bfloat16
VMEM = pl.BlockSpec(memory_space=pltpu.VMEM)
ANY = pl.BlockSpec(memory_space=pl.ANY)
NT = (((1,), (1,)), ((), ()))


def quarter_of(sx, px, count):
    return px + (sx % 2) * (count - 1 - 2 * px)


def cost(flops, moved):
    return pl.CostEstimate(flops=flops, bytes_accessed=moved, transcendentals=0)


def swap(array, axes, bit, count):
    return lax.ppermute(array, axes, [(i, i ^ bit) for i in range(count)])


def pair(index, kind):
    return index ^ 1 if kind == 0 else ((index + 1) ^ 1) - 1


def project_kernel(group, count, order, flat_ref, *refs):
    pieces, (whole_ref, own_ref), sends = refs[: len(order)], refs[len(order) : len(order) + 2], refs[len(order) + 2 :]
    me = lax.axis_index("sx") * group[1] + lax.axis_index("sy")
    sx, px = lax.axis_index("sx"), lax.axis_index("px")
    for bit, piece in zip(order, pieces):
        width = piece.shape[0]
        whole_ref[pl.ds(pl.multiple_of((me ^ bit) * width, width), width), :] = piece[...]
    rows = own_ref.shape[0]
    for k in range(count - 1, -1, -1):
        start = pl.multiple_of(quarter_of(sx, px ^ k, count) * rows, rows)
        part = lax.dot_general(flat_ref[pl.ds(start, rows), :], whole_ref[...], NT, preferred_element_type=F32)
        if k == 0:
            own_ref[...] = part
        else:
            sends[k - 1][...] = part.astype(BF16)


def sum_kernel(line, width, sides, valid_ref, own_ref, *refs):
    count = len(refs) - 2 - len(sides)
    parts, (coef_ref, mark_ref), strips = refs[:count], refs[count : count + 2], refs[count + 2 :]
    total = own_ref[...]
    for part in parts:
        total = total + part[...].astype(F32)
    coef_ref[...] = total
    mark = jnp.where(valid_ref[...] != 0.0, total, OFF).astype(BF16)
    mark_ref[...] = mark
    sy = lax.axis_index("sy")
    rows = mark.shape[0]
    slot = lax.broadcasted_iota(jnp.int32, (STRIP, rows), 0)
    spot = lax.broadcasted_iota(jnp.int32, (STRIP, rows), 1)
    line_of, col_of = slot // RADIUS, slot % RADIUS
    for kind, strip in zip(sides, strips):
        base = jnp.where(pair(sy, kind) > sy, width - RADIUS, 0)
        pick = (spot == line_of * width + col_of + base) & (slot < line * RADIUS)
        strip[...] = jnp.dot(pick.astype(BF16), mark, preferred_element_type=F32).astype(BF16)


def blend_kernel(coef_ref, factor_ref, band_ref, *refs):
    pieces, (average_ref, near_ref) = refs[:-2], refs[-2:]
    start = 0
    for piece in pieces:
        near_ref[start : start + piece.shape[0], :] = piece[...]
        start += piece.shape[0]
    if start < near_ref.shape[0]:
        near_ref[start:, :] = jnp.zeros((near_ref.shape[0] - start, near_ref.shape[1]), BF16)
    coef = coef_ref[...]
    here = coef.astype(BF16)
    wide = here.astype(F32)
    near = near_ref[...]
    far = near.astype(F32)
    inner = lax.dot_general(here, near, NT, preferred_element_type=F32)
    size_here = jnp.sum(wide * wide, axis=1, keepdims=True)
    ones = jnp.ones((8, far.shape[1]), F32)
    size_near = lax.dot_general(ones, far * far, NT, precision=lax.Precision.HIGHEST, preferred_element_type=F32)
    gap = jnp.maximum(size_here + size_near[:1] - 2.0 * inner, 0.0)
    weight = (jnp.exp(-gap * factor_ref[...]) * band_ref[...]).astype(BF16)
    total = 1.0 + jnp.sum(weight.astype(F32), axis=1, keepdims=True)
    numerator = coef + jnp.dot(weight, near, preferred_element_type=F32)
    average_ref[...] = (numerator / total).astype(BF16)


def rebuild_kernel(count, k, average_ref, whole_ref, *refs):
    out_ref, stage, sems = refs[-3:]
    rows = average_ref.shape[0]
    start = pl.multiple_of(quarter_of(lax.axis_index("sx"), lax.axis_index("px") ^ k, count) * rows, rows)
    chunks = sems.shape[0]
    step = whole_ref.shape[1] // chunks
    copies = []
    for i in range(chunks):
        cols = slice(i * step, (i + 1) * step)
        stage[:, cols] = jnp.dot(average_ref[...], whole_ref[:, cols], preferred_element_type=F32).astype(BF16)
        copies.append(pltpu.make_async_copy(stage.at[:, cols], out_ref.at[pl.ds(start, rows), cols], sems.at[i]))
        copies[-1].start()
    for copy in copies:
        copy.wait()


def rebuild(average, whole, out, shape, count, k):
    rows, rank = average.shape
    pixels = whole.shape[1]
    chunks = 3 if pixels % 384 == 0 else 1
    more = () if out is None else (out,)
    return pl.pallas_call(
        functools.partial(rebuild_kernel, count, k),
        out_shape=jax.ShapeDtypeStruct(shape, BF16),
        in_specs=[VMEM, VMEM] + [ANY] * len(more),
        out_specs=ANY,
        scratch_shapes=[pltpu.VMEM((rows, pixels), BF16), pltpu.SemaphoreType.DMA((chunks,))],
        input_output_aliases={2: 0} if more else {},
        cost_estimate=cost(2 * rows * rank * pixels, 2 * rows * pixels),
    )(average, whole, *more)


def gather_basis(shard, group):
    total = group[0] * group[1]
    if total != 8:
        whole = lax.all_gather(shard, ("sx", "sy"), axis=0, tiled=True)
        return None, [whole]
    held = {0: shard}
    core = group[1]
    held[core] = swap(shard, ("sx", "sy"), core, total)
    others = [bit for bit in range(1, total) if not bit & core]
    others.sort(key=lambda bit: bit.bit_count())
    for bit in others:
        held[bit] = swap(shard, ("sx", "sy"), bit, total)
    for bit in others:
        held[bit ^ core] = swap(held[bit], ("sx", "sy"), core, total)
    return tuple(held), list(held.values())


def band_of(group, count, line, width, kinds, sides, rows_near):
    sx, sy, px = lax.axis_index("sx"), lax.axis_index("sy"), lax.axis_index("px")
    v = sx * count + quarter_of(sx, px, count)
    total = group[0] * count
    spot = jnp.arange(line * width, dtype=jnp.int32)
    x_here, y_here = v * line + spot // width, sy * width + spot % width
    xs, ys = [x_here], [y_here]
    for kind in kinds:
        other = pair(v, kind)
        there = (other >= 0) & (other < total)
        xs.append(jnp.where(there, other * line + spot // width, -1000))
        ys.append(y_here)
    slot = jnp.arange(STRIP, dtype=jnp.int32)
    used = slot < line * RADIUS
    for side in sides:
        beside = pair(sy, side)
        base = jnp.where(beside > sy, 0, width - RADIUS)
        for kind in (None,) + kinds:
            other = v if kind is None else pair(v, kind)
            there = (other >= 0) & (other < total) & (beside >= 0) & (beside < group[1]) & used
            xs.append(jnp.where(there, other * line + slot // RADIUS, -1000))
            ys.append(beside * width + base + slot % RADIUS)
    x_near, y_near = jnp.concatenate(xs), jnp.concatenate(ys)
    short = rows_near - x_near.shape[0]
    x_near = jnp.pad(x_near, (0, short), constant_values=-1000)
    y_near = jnp.pad(y_near, (0, short))
    dx, dy = x_here[:, None] - x_near[None], y_here[:, None] - y_near[None]
    inside = (jnp.abs(dx) <= RADIUS) & (jnp.abs(dy) <= RADIUS) & ((dx != 0) | (dy != 0))
    return inside.astype(F32)


def line_pairs(kind, group, count):
    total = group[0] * count
    pairs = []
    for v in range(total):
        other = pair(v, kind)
        if 0 <= other < total:
            pairs.append((v, other))
    return pairs


def place(v, count):
    sx, q = divmod(v, count)
    return sx, quarter_of(sx, q, count)


def neighbour_swap(array, group, count, kind, side):
    lines = [(v, v) for v in range(group[0] * count)] if kind is None else line_pairs(kind, group, count)
    pairs = []
    for v, other in lines:
        for sy in range(group[1]):
            beside = sy if side is None else pair(sy, side)
            if 0 <= beside < group[1]:
                sx_a, px_a = place(v, count)
                sx_b, px_b = place(other, count)
                pairs.append(((sx_a * group[1] + sy) * count + px_a, (sx_b * group[1] + beside) * count + px_b))
    return lax.ppermute(array, ("sx", "sy", "px"), pairs)


def on_device(group, count, patterns, basis, valid, strength):
    cells_x, width, pixels = patterns.shape
    line = cells_x // count
    rows = line * width
    assert line * count == cells_x and line >= RADIUS and line * RADIUS <= STRIP
    sx, px = lax.axis_index("sx"), lax.axis_index("px")
    flat = patterns.reshape(cells_x * width, pixels)
    order, pieces = gather_basis(basis.T, group)
    if order is None:
        order, rank = (0,), pieces[0].shape[0]
        inner_group = (1, 0)
    else:
        rank, inner_group = pieces[0].shape[0] * len(pieces), group

    own_first = quarter_of(sx, px, count) * line
    valid_col = lax.dynamic_slice_in_dim(valid, own_first, line, 0).astype(F32).reshape(rows, 1)
    strength_col = lax.dynamic_slice_in_dim(strength, own_first, line, 0).reshape(rows, 1)
    factor_col = 1.0 / (2.0 * (pixels * count) * strength_col)
    kinds = (0, 1) if group[0] * count > 2 else (0,)
    sides = () if group[1] == 1 else (0,) if group[1] == 2 else (0, 1)
    rows_near = rows * (1 + len(kinds)) + STRIP * len(sides) * (1 + len(kinds))
    rows_near = -(-rows_near // 128) * 128
    band = band_of(group, count, line, width, kinds, sides, rows_near)

    body = functools.partial(project_kernel, group, count, order)
    if len(order) == 1:
        body = functools.partial(project_whole, count)
    whole, own, *sends = pl.pallas_call(
        body,
        out_shape=[
            jax.ShapeDtypeStruct((rank, pixels), BF16),
            jax.ShapeDtypeStruct((rows, rank), F32),
        ]
        + [jax.ShapeDtypeStruct((rows, rank), BF16)] * (count - 1),
        in_specs=[VMEM] * (1 + len(pieces)),
        out_specs=[VMEM] * (1 + count),
        cost_estimate=cost(2 * count * rows * rank * pixels, 2 * count * rows * pixels),
    )(flat, *pieces)
    parts = [swap(send, "px", k + 1, count) for k, send in enumerate(sends)]

    coef, mark, *strips = pl.pallas_call(
        functools.partial(sum_kernel, line, width, sides),
        out_shape=[jax.ShapeDtypeStruct((rows, rank), F32), jax.ShapeDtypeStruct((rows, rank), BF16)]
        + [jax.ShapeDtypeStruct((STRIP, rank), BF16)] * len(sides),
        in_specs=[VMEM] * (2 + len(parts)),
        out_specs=[VMEM] * (2 + len(sides)),
        cost_estimate=cost(8 * rows * rank, 16 * rows * rank),
    )(valid_col, own, *parts)
    near = [mark] + [neighbour_swap(mark, group, count, kind, None) for kind in kinds]
    for side, strip in zip(sides, strips):
        for kind in (None,) + kinds:
            near.append(neighbour_swap(strip, group, count, kind, side))

    average = pl.pallas_call(
        blend_kernel,
        out_shape=jax.ShapeDtypeStruct((rows, rank), BF16),
        in_specs=[VMEM] * (3 + len(near)),
        out_specs=VMEM,
        scratch_shapes=[pltpu.VMEM((rows_near, rank), BF16)],
        cost_estimate=cost(4 * rows * rank * rows_near, 4 * rows * rows_near),
    )(coef, factor_col, band, *near)

    out = None
    averages = [average] + [swap(average, "px", k, count) for k in range(1, count)]
    for k, piece in enumerate(averages):
        out = rebuild(piece, whole, out, (cells_x * width, pixels), count, k)
    return out.reshape(cells_x, width, pixels)


def project_whole(count, flat_ref, piece_ref, whole_ref, own_ref, *sends):
    sx, px = lax.axis_index("sx"), lax.axis_index("px")
    whole_ref[...] = piece_ref[...]
    rows = own_ref.shape[0]
    for k in range(count):
        start = pl.multiple_of(quarter_of(sx, px ^ k, count) * rows, rows)
        part = lax.dot_general(flat_ref[pl.ds(start, rows), :], whole_ref[...], NT, preferred_element_type=F32)
        if k == 0:
            own_ref[...] = part
        else:
            sends[k - 1][...] = part.astype(BF16)


def solution(mesh):
    group, count = (mesh.shape["sx"], mesh.shape["sy"]), mesh.shape["px"]
    return jax.shard_map(
        functools.partial(on_device, group, count),
        mesh=mesh,
        in_specs=(P("sx", "sy", "px"), P("px", ("sx", "sy")), P("sx", "sy"), P("sx", "sy")),
        out_specs=P("sx", "sy", "px"),
        check_vma=False,
    )
```

```python
import functools

import jax
import jax.numpy as jnp
from jax import lax
from jax.experimental import pallas as pl
from jax.experimental.pallas import tpu as pltpu
from jax.sharding import PartitionSpec as P


RADIUS = 3
STRIP = 16
OFF = 2.0**40
F32, BF16 = jnp.float32, jnp.bfloat16
VMEM = pl.BlockSpec(memory_space=pltpu.VMEM)
ANY = pl.BlockSpec(memory_space=pl.ANY)
NT = (((1,), (1,)), ((), ()))


def quarter_of(sx, px, count):
    return px + (sx % 2) * (count - 1 - 2 * px)


def grant(mib):
    return pltpu.CompilerParams(vmem_limit_bytes=mib << 20)


def cost(flops, moved):
    return pl.CostEstimate(flops=flops, bytes_accessed=moved, transcendentals=0)


def swap(array, axes, bit, count):
    return lax.ppermute(array, axes, [(i, i ^ bit) for i in range(count)])


def pair(index, kind):
    return index ^ 1 if kind == 0 else ((index + 1) ^ 1) - 1


def load_kernel(*refs):
    half = len(refs) // 3
    copies = [
        pltpu.make_async_copy(refs[i], refs[half + i], refs[2 * half + i]) for i in range(half)
    ]
    for copy in copies:
        copy.start()
    for copy in copies:
        copy.wait()


def load(*arrays):
    return pl.pallas_call(
        load_kernel,
        out_shape=[jax.ShapeDtypeStruct(a.shape, a.dtype) for a in arrays],
        in_specs=[ANY] * len(arrays),
        out_specs=[VMEM] * len(arrays),
        scratch_shapes=[pltpu.SemaphoreType.DMA] * len(arrays),
        compiler_params=grant(6),
        cost_estimate=cost(3_000_000_000, sum(a.size * 2 for a in arrays)),
    )(*arrays)


def project_kernel(group, count, order, flat_ref, *refs):
    pieces, (whole_ref, own_ref), sends = refs[: len(order)], refs[len(order) : len(order) + 2], refs[len(order) + 2 :]
    me = lax.axis_index("sx") * group[1] + lax.axis_index("sy")
    sx, px = lax.axis_index("sx"), lax.axis_index("px")
    for bit, piece in zip(order, pieces):
        width = piece.shape[0]
        whole_ref[pl.ds(pl.multiple_of((me ^ bit) * width, width), width), :] = piece[...]
    rows = own_ref.shape[0]
    for k in range(count - 1, -1, -1):
        start = pl.multiple_of(quarter_of(sx, px ^ k, count) * rows, rows)
        part = lax.dot_general(flat_ref[pl.ds(start, rows), :], whole_ref[...], NT, preferred_element_type=F32)
        if k == 0:
            own_ref[...] = part
        else:
            sends[k - 1][...] = part.astype(BF16)


def sum_kernel(line, width, sides, valid_ref, own_ref, *refs):
    count = len(refs) - 2 - len(sides)
    parts, (coef_ref, mark_ref), strips = refs[:count], refs[count : count + 2], refs[count + 2 :]
    total = own_ref[...]
    for part in parts:
        total = total + part[...].astype(F32)
    coef_ref[...] = total
    mark = jnp.where(valid_ref[...] != 0.0, total, OFF).astype(BF16)
    mark_ref[...] = mark
    sy = lax.axis_index("sy")
    rows = mark.shape[0]
    slot = lax.broadcasted_iota(jnp.int32, (STRIP, rows), 0)
    spot = lax.broadcasted_iota(jnp.int32, (STRIP, rows), 1)
    line_of, col_of = slot // RADIUS, slot % RADIUS
    for kind, strip in zip(sides, strips):
        base = jnp.where(pair(sy, kind) > sy, width - RADIUS, 0)
        pick = (spot == line_of * width + col_of + base) & (slot < line * RADIUS)
        strip[...] = jnp.dot(pick.astype(BF16), mark, preferred_element_type=F32).astype(BF16)


def blend_kernel(coef_ref, factor_ref, band_ref, *refs):
    pieces, (average_ref, near_ref) = refs[:-2], refs[-2:]
    start = 0
    for piece in pieces:
        near_ref[start : start + piece.shape[0], :] = piece[...]
        start += piece.shape[0]
    if start < near_ref.shape[0]:
        near_ref[start:, :] = jnp.zeros((near_ref.shape[0] - start, near_ref.shape[1]), BF16)
    coef = coef_ref[...]
    here = coef.astype(BF16)
    wide = here.astype(F32)
    near = near_ref[...]
    far = near.astype(F32)
    inner = lax.dot_general(here, near, NT, preferred_element_type=F32)
    size_here = jnp.sum(wide * wide, axis=1, keepdims=True)
    ones = jnp.ones((8, far.shape[1]), F32)
    size_near = lax.dot_general(ones, far * far, NT, precision=lax.Precision.HIGHEST, preferred_element_type=F32)
    gap = jnp.maximum(size_here + size_near[:1] - 2.0 * inner, 0.0)
    weight = (jnp.exp(-gap * factor_ref[...]) * band_ref[...]).astype(BF16)
    total = 1.0 + jnp.sum(weight.astype(F32), axis=1, keepdims=True)
    numerator = coef + jnp.dot(weight, near, preferred_element_type=F32)
    average_ref[...] = (numerator / total).astype(BF16)


def rebuild_kernel(count, ks, whole_ref, *refs):
    out_ref, stage, sems = refs[-3:]
    rows = refs[0].shape[0]
    sx, px = lax.axis_index("sx"), lax.axis_index("px")
    parts, chunks = sems.shape
    step = whole_ref.shape[1] // chunks
    held = [ref[...] for ref in refs[:parts]]
    left = held[0] if parts == 1 else jnp.concatenate(held, axis=0)
    copies = []
    for i in range(chunks):
        cols = slice(i * step, (i + 1) * step)
        stage[:, cols] = jnp.dot(left, whole_ref[:, cols], preferred_element_type=F32).astype(BF16)
        for j, k in enumerate(ks):
            start = pl.multiple_of(quarter_of(sx, px ^ k, count) * rows, rows)
            source = stage.at[j * rows : (j + 1) * rows, cols]
            copies.append(pltpu.make_async_copy(source, out_ref.at[pl.ds(start, rows), cols], sems.at[j, i]))
            copies[-1].start()
    for copy in copies:
        copy.wait()


def rebuild(averages, ks, whole, out, shape, count):
    rows, rank = averages[0].shape
    pixels = whole.shape[1]
    chunks = 3 if pixels % 384 == 0 else 1
    more = () if out is None else (out,)
    return pl.pallas_call(
        functools.partial(rebuild_kernel, count, ks),
        out_shape=jax.ShapeDtypeStruct(shape, BF16),
        in_specs=[VMEM] * (1 + len(ks)) + [ANY] * len(more),
        out_specs=ANY,
        scratch_shapes=[pltpu.VMEM((rows * len(ks), pixels), BF16), pltpu.SemaphoreType.DMA((len(ks), chunks))],
        input_output_aliases={1 + len(ks): 0} if more else {},
        compiler_params=grant(6),
        cost_estimate=cost(2 * rows * len(ks) * rank * pixels, 2 * rows * len(ks) * pixels),
    )(whole, *averages, *more)


def gather_basis(shard, group):
    total = group[0] * group[1]
    if total != 8:
        whole = lax.all_gather(shard, ("sx", "sy"), axis=0, tiled=True)
        return None, [whole]
    held = {0: shard}
    core = group[1]
    held[core] = swap(shard, ("sx", "sy"), core, total)
    others = [bit for bit in range(1, total) if not bit & core]
    others.sort(key=lambda bit: bit.bit_count())
    for bit in others:
        held[bit] = swap(shard, ("sx", "sy"), bit, total)
    for bit in others:
        held[bit ^ core] = swap(held[bit], ("sx", "sy"), core, total)
    return tuple(held), list(held.values())


def band_of(group, count, line, width, kinds, sides, rows_near):
    sx, sy, px = lax.axis_index("sx"), lax.axis_index("sy"), lax.axis_index("px")
    v = sx * count + quarter_of(sx, px, count)
    total = group[0] * count
    spot = jnp.arange(line * width, dtype=jnp.int32)
    x_here, y_here = v * line + spot // width, sy * width + spot % width
    xs, ys = [], []
    slot = jnp.arange(STRIP, dtype=jnp.int32)
    used = slot < line * RADIUS
    for kind in (None,) + kinds:
        other = v if kind is None else pair(v, kind)
        there = (other >= 0) & (other < total)
        xs.append(jnp.where(there, other * line + spot // width, -1000))
        ys.append(y_here)
        for side in sides:
            beside = pair(sy, side)
            base = jnp.where(beside > sy, 0, width - RADIUS)
            known = there & (beside >= 0) & (beside < group[1]) & used
            xs.append(jnp.where(known, other * line + slot // RADIUS, -1000))
            ys.append(beside * width + base + slot % RADIUS)
    x_near, y_near = jnp.concatenate(xs), jnp.concatenate(ys)
    short = rows_near - x_near.shape[0]
    x_near = jnp.pad(x_near, (0, short), constant_values=-1000)
    y_near = jnp.pad(y_near, (0, short))
    dx, dy = x_here[:, None] - x_near[None], y_here[:, None] - y_near[None]
    inside = (jnp.abs(dx) <= RADIUS) & (jnp.abs(dy) <= RADIUS) & ((dx != 0) | (dy != 0))
    return inside.astype(F32)


def line_pairs(kind, group, count):
    total = group[0] * count
    pairs = []
    for v in range(total):
        other = pair(v, kind)
        if 0 <= other < total:
            pairs.append((v, other))
    return pairs


def place(v, count):
    sx, q = divmod(v, count)
    return sx, quarter_of(sx, q, count)


def neighbour_swap(array, group, count, kind, side):
    lines = [(v, v) for v in range(group[0] * count)] if kind is None else line_pairs(kind, group, count)
    pairs = []
    for v, other in lines:
        for sy in range(group[1]):
            beside = sy if side is None else pair(sy, side)
            if 0 <= beside < group[1]:
                sx_a, px_a = place(v, count)
                sx_b, px_b = place(other, count)
                pairs.append(((sx_a * group[1] + sy) * count + px_a, (sx_b * group[1] + beside) * count + px_b))
    return lax.ppermute(array, ("sx", "sy", "px"), pairs)


def on_device(group, count, patterns, basis, valid, strength):
    cells_x, width, pixels = patterns.shape
    line = cells_x // count
    rows = line * width
    assert line * count == cells_x and line >= RADIUS and line * RADIUS <= STRIP
    sx, px = lax.axis_index("sx"), lax.axis_index("px")
    flat = patterns.reshape(cells_x * width, pixels)
    shard = basis.T
    order, pieces = gather_basis(shard, group)
    if order is None:
        (flat,) = load(flat)
    else:
        flat, pieces[0] = load(flat, shard)
    if order is None:
        order, rank = (0,), pieces[0].shape[0]
    else:
        rank = pieces[0].shape[0] * len(pieces)

    own_first = quarter_of(sx, px, count) * line
    valid_col = lax.dynamic_slice_in_dim(valid, own_first, line, 0).astype(F32).reshape(rows, 1)
    strength_col = lax.dynamic_slice_in_dim(strength, own_first, line, 0).reshape(rows, 1)
    factor_col = 1.0 / (2.0 * (pixels * count) * strength_col)
    kinds = (0, 1) if group[0] * count > 2 else (0,)
    sides = () if group[1] == 1 else (0,) if group[1] == 2 else (0, 1)
    rows_near = rows * (1 + len(kinds)) + STRIP * len(sides) * (1 + len(kinds))
    rows_near = -(-rows_near // 128) * 128
    band = band_of(group, count, line, width, kinds, sides, rows_near)

    body = functools.partial(project_kernel, group, count, order)
    if len(order) == 1:
        body = functools.partial(project_whole, count)
    whole, own, *sends = pl.pallas_call(
        body,
        out_shape=[
            jax.ShapeDtypeStruct((rank, pixels), BF16),
            jax.ShapeDtypeStruct((rows, rank), F32),
        ]
        + [jax.ShapeDtypeStruct((rows, rank), BF16)] * (count - 1),
        in_specs=[VMEM] * (1 + len(pieces)),
        out_specs=[VMEM] * (1 + count),
        compiler_params=grant(16),
        cost_estimate=cost(2 * count * rows * rank * pixels, 2 * count * rows * pixels),
    )(flat, *pieces)
    parts = [swap(send, "px", k + 1, count) for k, send in enumerate(sends)]

    coef, mark, *strips = pl.pallas_call(
        functools.partial(sum_kernel, line, width, sides),
        out_shape=[jax.ShapeDtypeStruct((rows, rank), F32), jax.ShapeDtypeStruct((rows, rank), BF16)]
        + [jax.ShapeDtypeStruct((STRIP, rank), BF16)] * len(sides),
        in_specs=[VMEM] * (2 + len(parts)),
        out_specs=[VMEM] * (2 + len(sides)),
        compiler_params=grant(6),
        cost_estimate=cost(8 * rows * rank, 16 * rows * rank),
    )(valid_col, own, *parts)
    beside = [neighbour_swap(strip, group, count, None, side) for side, strip in zip(sides, strips)]
    mine = jnp.concatenate([mark] + beside, axis=0) if beside else mark
    near = [mine] + [neighbour_swap(mine, group, count, kind, None) for kind in kinds]

    average = pl.pallas_call(
        blend_kernel,
        out_shape=jax.ShapeDtypeStruct((rows, rank), BF16),
        in_specs=[VMEM] * (3 + len(near)),
        out_specs=VMEM,
        scratch_shapes=[pltpu.VMEM((rows_near, rank), BF16)],
        compiler_params=grant(6),
        cost_estimate=cost(4 * rows * rank * rows_near, 4 * rows * rows_near),
    )(coef, factor_col, band, *near)

    out = None
    averages = [average] + [swap(average, "px", k, count) for k in range(1, count)]
    for ks in rebuild_groups(count):
        out = rebuild([averages[k] for k in ks], ks, whole, out, (cells_x * width, pixels), count)
    return out.reshape(cells_x, width, pixels)


def rebuild_groups(count):
    return [(0,), (1,)] + [tuple(range(2, count))] if count > 2 else [(k,) for k in range(count)]


def project_whole(count, flat_ref, piece_ref, whole_ref, own_ref, *sends):
    sx, px = lax.axis_index("sx"), lax.axis_index("px")
    whole_ref[...] = piece_ref[...]
    rows = own_ref.shape[0]
    for k in range(count):
        start = pl.multiple_of(quarter_of(sx, px ^ k, count) * rows, rows)
        part = lax.dot_general(flat_ref[pl.ds(start, rows), :], whole_ref[...], NT, preferred_element_type=F32)
        if k == 0:
            own_ref[...] = part
        else:
            sends[k - 1][...] = part.astype(BF16)


def solution(mesh):
    group, count = (mesh.shape["sx"], mesh.shape["sy"]), mesh.shape["px"]

    def body(*arrays):
        return on_device(group, count, *arrays)

    return jax.shard_map(
        body,
        mesh=mesh,
        in_specs=(P("sx", "sy", "px"), P("px", ("sx", "sy")), P("sx", "sy"), P("sx", "sy")),
        out_specs=P("sx", "sy", "px"),
        check_vma=False,
    )
```
